16 devices in a mesh: dp: 2 (over z), tp: 8 (over y, x, core).
Axes of the slice: x: 2, y: 2, z: 2, core: 2. Of those that a mesh axis runs over, the one named last changes fastest.
Arguments:
- x_in: bfloat16 [4, 2048, 5120], P('dp', 'tp'), parts along dimension 0
- ln_gain: float32 [2, 5120], replicated
- ln_bias: float32 [2, 5120], replicated
- w_qkv: bfloat16 [2, 5120, 3, 40, 128], P(None, None, None, 'tp')
- w_out: bfloat16 [2, 40, 128, 5120], P(None, 'tp')
- b_out: float32 [2, 5120], replicated
- w_up: bfloat16 [2, 5120, 20480], P(None, None, 'tp')
- b_up: float32 [2, 20480], P(None, 'tp')
- w_down: bfloat16 [2, 20480, 5120], P(None, 'tp')
- b_down: float32 [2, 5120], replicated
Outputs:
- output: bfloat16 [4, 2048, 5120], P('dp', 'tp'), parts along dimension 0
There are 2 independent parts. The reference program is written for one: setup_inputs(seed, part) draws one part's arguments, and reference() takes and returns one part's arrays. A program takes and returns all parts, laid end to end along the dimension named above; an argument that names none is the same for every part.
All inputs are finite; a program needn't handle non-finite values.
Results may differ from the reference program's by a relative error of at most 0.0127431.
Values are sent between devices in bfloat16 or wider.
A program may use at most 1 GiB of HBM per device.

```python
import math
import jax
import jax.numpy as jnp
from jax import lax

BATCH_SIZE = 2
SEQ_LEN = 2048
MODEL_DIM = 5120
N_HEADS = 40
HEAD_DIM = 128
FFN_WIDTH = 20480
NUM_LAYERS = 2
LN_EPS = 1e-5


def setup_inputs(seed: int = 0, part: int = 0) -> dict:
    key = jax.random.key(seed)
    shared = jax.random.split(key, 9)
    part_keys = jax.random.split(jax.random.fold_in(key, part), 2)
    tok_scale = 0.5 + jax.random.uniform(part_keys[0], (BATCH_SIZE, SEQ_LEN, 1), jnp.float32)
    x_in = jax.random.normal(part_keys[1], (BATCH_SIZE, SEQ_LEN, MODEL_DIM), jnp.float32) * tok_scale
    logit_std = math.sqrt(max(math.log(SEQ_LEN / 32.0), 1.0))
    qk_gain = math.sqrt(logit_std)
    comp_gain = jnp.array([qk_gain, qk_gain, 1.0], jnp.float32).reshape(1, 1, 3, 1, 1)
    in_scale = MODEL_DIM ** -0.5
    w_qkv = jax.random.normal(shared[0], (NUM_LAYERS, MODEL_DIM, 3, N_HEADS, HEAD_DIM), jnp.float32) * (in_scale * comp_gain)
    w_out = jax.random.normal(shared[1], (NUM_LAYERS, N_HEADS, HEAD_DIM, MODEL_DIM), jnp.float32) * (1.5 * in_scale)
    w_up = jax.random.normal(shared[2], (NUM_LAYERS, MODEL_DIM, FFN_WIDTH), jnp.float32) * in_scale
    w_down = jax.random.normal(shared[3], (NUM_LAYERS, FFN_WIDTH, MODEL_DIM), jnp.float32) * FFN_WIDTH ** -0.5
    ln_gain = 1.0 + 0.2 * jax.random.normal(shared[4], (NUM_LAYERS, MODEL_DIM), jnp.float32)
    ln_bias = 0.2 * jax.random.normal(shared[5], (NUM_LAYERS, MODEL_DIM), jnp.float32)
    b_out = 0.1 * jax.random.normal(shared[6], (NUM_LAYERS, MODEL_DIM), jnp.float32)
    b_up = 0.3 * jax.random.normal(shared[7], (NUM_LAYERS, FFN_WIDTH), jnp.float32)
    b_down = 0.1 * jax.random.normal(shared[8], (NUM_LAYERS, MODEL_DIM), jnp.float32)
    return {
        'x_in': x_in.astype(jnp.bfloat16),
        'ln_gain': ln_gain,
        'ln_bias': ln_bias,
        'w_qkv': w_qkv.astype(jnp.bfloat16),
        'w_out': w_out.astype(jnp.bfloat16),
        'b_out': b_out,
        'w_up': w_up.astype(jnp.bfloat16),
        'b_up': b_up,
        'w_down': w_down.astype(jnp.bfloat16),
        'b_down': b_down,
    }


def layer_norm(residual, gain, bias):
    row_mean = jnp.mean(residual, axis=-1, keepdims=True)
    centered = residual - row_mean
    row_var = jnp.mean(centered * centered, axis=-1, keepdims=True)
    return (centered * lax.rsqrt(row_var + LN_EPS) * gain + bias).astype(jnp.bfloat16)


def query_block(batch, heads, q_len, k_len):
    block = q_len
    while block % 2 == 0 and block > 16 and batch * heads * block * k_len > 2 ** 24:
        block = block // 2
    return block


def causal_attention(queries, keys, values):
    batch, seq_len, heads, head_dim = queries.shape
    block = query_block(batch, heads, seq_len, seq_len)
    inv_sqrt = head_dim ** -0.5
    key_pos = jnp.arange(seq_len)
    keys_f = keys.astype(jnp.float32)
    values_f = values.astype(jnp.float32)

    def one_block(index):
        q_blk = lax.dynamic_slice_in_dim(queries, index * block, block, axis=1).astype(jnp.float32)
        scores = jnp.einsum('bqhe,bkhe->bhqk', q_blk, keys_f) * inv_sqrt
        q_pos = index * block + jnp.arange(block)
        scores = jnp.where(key_pos[None, :] <= q_pos[:, None], scores, -jnp.inf)
        attn_prob = jax.nn.softmax(scores, axis=-1).astype(jnp.bfloat16).astype(jnp.float32)
        return jnp.einsum('bhqk,bkhe->bqhe', attn_prob, values_f).astype(jnp.bfloat16)

    out_blocks = lax.map(one_block, jnp.arange(seq_len // block))
    return jnp.moveaxis(out_blocks, 0, 1).reshape(batch, seq_len, heads, head_dim)


def one_layer(residual, params):
    ln_gain, ln_bias, w_qkv, w_out, b_out, w_up, b_up, w_down, b_down = params
    normed = layer_norm(residual, ln_gain, ln_bias)
    normed_f = normed.astype(jnp.float32)
    qkv_all = jnp.einsum('bsd,dthe->bsthe', normed_f, w_qkv.astype(jnp.float32)).astype(jnp.bfloat16)
    attn_out = causal_attention(qkv_all[:, :, 0], qkv_all[:, :, 1], qkv_all[:, :, 2])
    attn_sum = jnp.einsum('bshe,hed->bsd', attn_out.astype(jnp.float32), w_out.astype(jnp.float32))
    hidden = jnp.einsum('bsd,df->bsf', normed_f, w_up.astype(jnp.float32)) + b_up
    gelu_out = jax.nn.gelu(hidden, approximate=True).astype(jnp.bfloat16)
    mlp_sum = jnp.einsum('bsf,fd->bsd', gelu_out.astype(jnp.float32), w_down.astype(jnp.float32))
    return residual + (attn_sum + mlp_sum + b_out + b_down), None


def reference(x_in, ln_gain, ln_bias, w_qkv, w_out, b_out, w_up, b_up, w_down, b_down):
    residual = x_in.astype(jnp.float32)
    residual, _ = lax.scan(one_layer, residual, (ln_gain, ln_bias, w_qkv, w_out, b_out, w_up, b_up, w_down, b_down))
    return residual.astype(jnp.bfloat16)
```

```python
import functools
import math

import jax
import jax.numpy as jnp
from jax import lax
from jax.experimental import pallas as pl
from jax.experimental.pallas import tpu as pltpu
from jax.sharding import PartitionSpec as P

LN_EPS = 1e-5
VMEM_LIMIT = 56 * 1024 * 1024
ANY = pl.BlockSpec(memory_space=pl.ANY)
PARAMS = pltpu.CompilerParams(vmem_limit_bytes=VMEM_LIMIT)


def norm_rows(row, gain, bias):
    row_mean = jnp.mean(row, axis=-1, keepdims=True)
    centered = row - row_mean
    row_var = jnp.mean(centered * centered, axis=-1, keepdims=True)
    return (centered * lax.rsqrt(row_var + LN_EPS) * gain + bias).astype(jnp.bfloat16)


def ln_kernel(token_ref, x_ref, gain_ref, bias_ref, h_ref):
    del token_ref
    h_ref[...] = norm_rows(x_ref[0].astype(jnp.float32), gain_ref[0], bias_ref[0])


def first_norm(token, x, seq, row, rows, ln_gain, ln_bias):
    width = x.shape[-1]
    tile = 32
    first = row // tile
    vec = pl.BlockSpec((1, 1, width), lambda i: (0, 0, 0))
    return pl.pallas_call(
        ln_kernel,
        grid=(rows // tile,),
        in_specs=[ANY, pl.BlockSpec((1, tile, width), lambda i: (seq, first + i, 0)), vec, vec],
        out_specs=pl.BlockSpec((tile, width), lambda i: (i, 0)),
        out_shape=jax.ShapeDtypeStruct((rows, width), jnp.bfloat16),
        compiler_params=PARAMS,
        cost_estimate=pl.CostEstimate(flops=rows * width * 20, bytes_accessed=rows * width * 4, transcendentals=0),
        name="first_norm",
    )(token, x, ln_gain, ln_bias)


def relay_kernel(token_ref, keep_ref, second_ref, out_ref):
    del token_ref
    out_ref[...] = (keep_ref[...] + second_ref[...].astype(jnp.float32)).astype(jnp.bfloat16)


def relay(token, keep, second):
    rows, width = keep.shape[0] // 2, keep.shape[1]
    tile = 64
    first = rows // tile
    data = pl.BlockSpec((tile, width), lambda i: (first + i, 0))
    return pl.pallas_call(
        relay_kernel,
        grid=(rows // tile,),
        in_specs=[ANY, data, data],
        out_specs=pl.BlockSpec((tile, width), lambda i: (i, 0)),
        out_shape=jax.ShapeDtypeStruct((rows, width), jnp.bfloat16),
        compiler_params=PARAMS,
        cost_estimate=pl.CostEstimate(flops=rows * width * 10, bytes_accessed=rows * width * 8, transcendentals=0),
        name="relay",
    )(token, keep, second)


def finish_kernel(last, raw, token_ref, keep_ref, second_ref, third_ref, res_ref, b_out_ref, b_down_ref, *rest):
    del token_ref
    summed = keep_ref[...] + second_ref[...].astype(jnp.float32) + third_ref[...].astype(jnp.float32)
    residual = res_ref[0].astype(jnp.float32) if raw else res_ref[...]
    row = residual + (summed + (b_out_ref[0] + b_down_ref[0]))
    if last:
        rest[0][...] = row.astype(jnp.bfloat16)
    else:
        gain_ref, bias_ref, new_res_ref, h_ref = rest
        new_res_ref[...] = row
        h_ref[...] = norm_rows(row, gain_ref[0], bias_ref[0])


def finish(token, layer_idx, last, keep, second, third, residual, raw, b_out, b_down, ln_gain, ln_bias):
    rows, width = third.shape
    tile = 32
    data = pl.BlockSpec((tile, width), lambda i: (i, 0))
    res_spec = data
    if raw is not None:
        seq, first = raw[0], raw[1] // tile
        res_spec = pl.BlockSpec((1, tile, width), lambda i: (seq, first + i, 0))
    vec = pl.BlockSpec((1, 1, width), lambda i: (layer_idx, 0, 0))
    next_vec = pl.BlockSpec((1, 1, width), lambda i: (layer_idx + 1, 0, 0))
    args = [token, keep, second, third, residual, b_out, b_down]
    in_specs = [ANY] + [data] * 3 + [res_spec] + [vec] * 2
    half = jax.ShapeDtypeStruct((rows, width), jnp.bfloat16)
    if last:
        out_shape, out_specs = half, data
    else:
        args += [ln_gain, ln_bias]
        in_specs += [next_vec] * 2
        out_shape, out_specs = (jax.ShapeDtypeStruct((rows, width), jnp.float32), half), (data, data)
    return pl.pallas_call(
        functools.partial(finish_kernel, last, raw is not None),
        grid=(rows // tile,),
        in_specs=in_specs,
        out_specs=out_specs,
        out_shape=out_shape,
        compiler_params=PARAMS,
        cost_estimate=pl.CostEstimate(flops=rows * width * 30, bytes_accessed=rows * width * 16, transcendentals=0),
        name="finish",
    )(*args)


SLICES = 4


def fetch(x_hbm, x_all, sems, k):
    step = x_all.shape[1] // SLICES
    part = pl.ds(k * step, step)
    return pltpu.make_async_copy(x_hbm.at[:, part], x_all.at[:, part], sems.at[k])


def sliced_matmul(x_hbm, x_all, sems, right, store):
    depth = x_all.shape[1]
    step = depth // SLICES

    @pl.when(pl.program_id(0) == 0)
    def _():
        for k in range(SLICES):
            fetch(x_hbm, x_all, sems, k).start()
        total = None
        for k in range(SLICES):
            fetch(x_hbm, x_all, sems, k).wait()
            term = jnp.dot(x_all[:, k * step:(k + 1) * step], right(k * step, step), preferred_element_type=jnp.float32)
            total = term if total is None else total + term
        store(total)

    @pl.when(pl.program_id(0) > 0)
    def _():
        store(jnp.dot(x_all[...], right(0, depth), preferred_element_type=jnp.float32))


def qkv_kernel(group, token_ref, x_hbm, w_ref, out_ref, x_all, sems):
    del token_ref
    head_dim = w_ref.shape[-1]

    def right(start, size):
        return jnp.concatenate([w_ref[0, i, start:start + size, :] for i in range(group)], axis=1)

    def store(value):
        for i in range(group):
            out_ref[i] = value[:, i * head_dim:(i + 1) * head_dim].astype(jnp.bfloat16)

    sliced_matmul(x_hbm, x_all, sems, right, store)


def qkv_project(token, layer_idx, x, w_qkv):
    rows, depth = x.shape
    _, slabs, _, head_dim = w_qkv.shape
    group = 4
    return pl.pallas_call(
        functools.partial(qkv_kernel, group),
        grid=(pl.cdiv(slabs, group),),
        in_specs=[ANY, ANY, pl.BlockSpec((1, group, depth, head_dim), lambda j: (layer_idx, j, 0, 0))],
        out_specs=pl.BlockSpec((group, rows, head_dim), lambda j: (j, 0, 0)),
        out_shape=jax.ShapeDtypeStruct((slabs, rows, head_dim), jnp.bfloat16),
        scratch_shapes=[pltpu.VMEM((rows, depth), jnp.bfloat16), pltpu.SemaphoreType.DMA((SLICES,))],
        compiler_params=PARAMS,
        cost_estimate=pl.CostEstimate(flops=2 * rows * depth * slabs * head_dim, bytes_accessed=2 * depth * slabs * head_dim,
                                      transcendentals=0),
        name="qkv_project",
    )(token, x, w_qkv)


def up_kernel(token_ref, x_hbm, w_ref, b_ref, out_ref, x_all, sems):
    del token_ref

    def store(value):
        hidden = value + b_ref[0]
        inner = math.sqrt(2 / math.pi) * (hidden + 0.044715 * (hidden * hidden * hidden))
        out_ref[...] = (hidden * (0.5 * (1.0 + jnp.tanh(inner)))).astype(jnp.bfloat16)

    sliced_matmul(x_hbm, x_all, sems, lambda start, size: w_ref[0, start:start + size, :], store)


def up_project(token, layer_idx, x, w_up, b_up):
    rows, depth = x.shape
    width = w_up.shape[-1]
    tile = 512
    return pl.pallas_call(
        up_kernel,
        grid=(width // tile,),
        in_specs=[ANY, ANY, pl.BlockSpec((1, depth, tile), lambda j: (layer_idx, 0, j)),
                  pl.BlockSpec((1, 1, tile), lambda j: (layer_idx, 0, j))],
        out_specs=pl.BlockSpec((rows, tile), lambda j: (0, j)),
        out_shape=jax.ShapeDtypeStruct((rows, width), jnp.bfloat16),
        scratch_shapes=[pltpu.VMEM((rows, depth), jnp.bfloat16), pltpu.SemaphoreType.DMA((SLICES,))],
        compiler_params=PARAMS,
        cost_estimate=pl.CostEstimate(flops=2 * rows * depth * width, bytes_accessed=2 * depth * width,
                                      transcendentals=rows * width),
        name="up_project",
    )(token, x, w_up, b_up)


def attention_kernel(n_chunks, q_tile, token_ref, *refs):
    del token_ref
    parts = [refs[3 * c:3 * c + 3] for c in range(n_chunks)]
    out_ref, q_all, k_all, v_all = refs[3 * n_chunks:]
    for c in range(n_chunks):
        for whole, part in zip((q_all, k_all, v_all), parts[c]):
            whole[:, c] = part[0]
    blocks, _, rows, head_dim = q_all.shape
    seq_len = blocks * n_chunks * rows
    exp_scale = head_dim ** -0.5 * math.log2(math.e)
    queries = q_all[...].reshape(seq_len, head_dim)
    keys = k_all[...].reshape(seq_len, head_dim)
    values = v_all[...].reshape(seq_len, head_dim)
    causal = (lax.broadcasted_iota(jnp.int32, (q_tile, q_tile), 1) <= lax.broadcasted_iota(jnp.int32, (q_tile, q_tile), 0))
    nt = (((1,), (1,)), ((), ()))
    for tile in range(seq_len // q_tile):
        start, stop = tile * q_tile, (tile + 1) * q_tile
        query = queries[start:stop]
        diag = lax.dot_general(query, keys[start:stop], nt, preferred_element_type=jnp.float32)
        diag = jnp.where(causal, diag, -jnp.inf)
        top = jnp.max(diag, axis=1, keepdims=True)
        if tile:
            past = lax.dot_general(query, keys[:start], nt, preferred_element_type=jnp.float32)
            top = jnp.maximum(top, jnp.max(past, axis=1, keepdims=True))
        diag = jnp.exp2((diag - top) * exp_scale)
        total = jnp.sum(diag, axis=1, keepdims=True)
        if tile:
            past = jnp.exp2((past - top) * exp_scale)
            total = total + jnp.sum(past, axis=1, keepdims=True)
        inverse = 1.0 / total
        out = jnp.dot((diag * inverse).astype(jnp.bfloat16), values[start:stop], preferred_element_type=jnp.float32)
        if tile:
            out = out + jnp.dot((past * inverse).astype(jnp.bfloat16), values[:start], preferred_element_type=jnp.float32)
        out_ref[start:stop, :] = out.astype(jnp.bfloat16)


def attention(token, qkv_chunks, blocks):
    n_chunks = len(qkv_chunks)
    slabs, all_rows, head_dim = qkv_chunks[0].shape
    heads, rows = slabs // 3, all_rows // blocks
    seq_len = all_rows * n_chunks
    specs = [pl.BlockSpec((1, blocks, rows, head_dim), lambda h, t=t: (t * heads + h, 0, 0, 0)) for t in range(3)]
    args = [chunk.reshape(slabs, blocks, rows, head_dim) for chunk in qkv_chunks for _ in range(3)]
    whole = pltpu.VMEM((blocks, n_chunks, rows, head_dim), jnp.bfloat16)
    return pl.pallas_call(
        functools.partial(attention_kernel, n_chunks, 256),
        grid=(heads,),
        in_specs=[ANY] + specs * n_chunks,
        out_specs=pl.BlockSpec((seq_len, head_dim), lambda h: (0, h)),
        out_shape=jax.ShapeDtypeStruct((seq_len, heads * head_dim), jnp.bfloat16),
        scratch_shapes=[whole] * 3,
        compiler_params=PARAMS,
        cost_estimate=pl.CostEstimate(flops=heads * seq_len * seq_len * head_dim * 8,
                                      bytes_accessed=heads * seq_len * head_dim * 8, transcendentals=0),
        name="attention",
    )(token, *args)


def project_kernel(n_sub, mine, table_ref, token_ref, *refs):
    del table_ref, token_ref
    n_u = 4 * n_sub
    u_refs, o_refs, refs = refs[:n_u], refs[n_u:n_u + 4], refs[n_u + 4:]
    w_down_ref, w_out_ref, refs = refs[0], refs[1], refs[2:]
    lhs_u, lhs_o = refs[-2:]

    @pl.when(pl.program_id(0) == 0)
    def _():
        rows = u_refs[0].shape[0]
        for k in range(n_u):
            lhs_u[k * rows:(k + 1) * rows, :] = u_refs[k][...]
        rows = o_refs[0].shape[2]
        for k in range(4):
            lhs_o[k * rows:(k + 1) * rows, :] = o_refs[k][0, 0]

    partial = jnp.dot(lhs_u[...], w_down_ref[0], preferred_element_type=jnp.float32)
    partial = partial + jnp.dot(lhs_o[...], w_out_ref[0], preferred_element_type=jnp.float32)
    if mine:
        first_ref, keep_ref, send_ref = refs[:3]
        partial = partial + first_ref[...].astype(jnp.float32)
        half = partial.shape[0] // 2
        keep_ref[...] = partial[:half]
        send_ref[...] = partial[half:].astype(jnp.bfloat16)
    else:
        refs[0][...] = partial.astype(jnp.bfloat16)


def project(token, layer_idx, chunk, n_chunks, table, u_parts, attn_out, w_down, w_out, first=None):
    n_sub = len(u_parts)
    rows = u_parts[0].shape[0] // 8
    depth, width = w_down.shape[1:]
    heads_width = attn_out.shape[1]
    chunk_rows = rows * n_sub
    attn_blocks = attn_out.reshape(8, n_chunks, chunk_rows, heads_width)
    tile = 512
    in_specs, args = [ANY], [token]
    for k in range(4):
        for part in u_parts:
            in_specs.append(pl.BlockSpec((rows, depth), lambda j, tbl, k=k: (tbl[k], 0)))
            args.append(part)
    for k in range(4):
        in_specs.append(pl.BlockSpec((1, 1, chunk_rows, heads_width), lambda j, tbl, k=k: (tbl[k], chunk, 0, 0)))
        args.append(attn_blocks)
    in_specs.append(pl.BlockSpec((1, depth, tile), lambda j, tbl: (layer_idx, 0, j)))
    in_specs.append(pl.BlockSpec((1, heads_width, tile), lambda j, tbl: (layer_idx, 0, j)))
    args += [w_down, w_out]
    all_rows = 4 * chunk_rows
    if first is None:
        out_shape = jax.ShapeDtypeStruct((all_rows, width), jnp.bfloat16)
        out_specs = pl.BlockSpec((all_rows, tile), lambda j, tbl: (0, j))
    else:
        in_specs.append(pl.BlockSpec((all_rows, tile), lambda j, tbl: (0, j)))
        args.append(first)
        out_shape = (jax.ShapeDtypeStruct((all_rows // 2, width), jnp.float32),
                     jax.ShapeDtypeStruct((all_rows // 2, width), jnp.bfloat16))
        out_specs = (pl.BlockSpec((all_rows // 2, tile), lambda j, tbl: (0, j)),) * 2
    return pl.pallas_call(
        functools.partial(project_kernel, n_sub, first is not None),
        grid_spec=pltpu.PrefetchScalarGridSpec(
            num_scalar_prefetch=1,
            grid=(width // tile,),
            in_specs=in_specs,
            out_specs=out_specs,
            scratch_shapes=[pltpu.VMEM((all_rows, depth), jnp.bfloat16), pltpu.VMEM((all_rows, heads_width), jnp.bfloat16)],
        ),
        out_shape=out_shape,
        compiler_params=PARAMS,
        cost_estimate=pl.CostEstimate(flops=2 * all_rows * (depth + heads_width) * width,
                                      bytes_accessed=2 * (depth + heads_width) * width, transcendentals=0),
        name="project",
    )(table, *args)


def solution(mesh):
    tp_size = mesh.shape['tp']
    act_spec = P('dp', 'tp', None)
    partner = [(i, i ^ 1) for i in range(tp_size)]
    hop_one = [(i, i ^ (2 if i & 1 else 4)) for i in range(tp_size)]
    hop_two = [(i, i ^ (4 if i & 1 else 2)) for i in range(tp_size)]

    def local_fn(x_in, ln_gain, ln_bias, w_qkv, w_out, b_out, w_up, b_up, w_down, b_down):
        batch, local_rows, width = x_in.shape
        n_layers, _, _, heads, head_dim = w_qkv.shape
        vec = lambda a: a.reshape(n_layers, 1, a.shape[1])
        ln_gain, ln_bias, b_out, b_down, b_up = vec(ln_gain), vec(ln_bias), vec(b_out), vec(b_down), vec(b_up)
        w_out = w_out.reshape(n_layers, heads * head_dim, width)
        w_qkv = jnp.transpose(w_qkv, (0, 2, 3, 1, 4)).reshape(n_layers, 3 * heads, width, head_dim)
        me = lax.axis_index('tp').astype(jnp.int32)
        bit_one = jnp.where((me & 1) == 1, 2, 4)
        bit_two = 6 - bit_one
        steps = jnp.array([0, 0, 1, 1], jnp.int32), jnp.array([0, 1, 0, 1], jnp.int32)
        mine_table = (me ^ (steps[0] * bit_one) ^ (steps[1] * bit_two)).astype(jnp.int32)
        other_table = (me ^ 1 ^ (steps[0] * bit_two) ^ (steps[1] * bit_one)).astype(jnp.int32)

        n_chunks = 2
        chunk_rows = local_rows // n_chunks
        token = [x_in]

        def gather(h):
            return lax.all_gather(h, 'tp', axis=0, tiled=True)

        residual, gathered = {}, {}
        for s in range(batch):
            n_sub = 2 if s == 0 else 1
            sub_rows = chunk_rows // n_sub
            for c in range(n_chunks):
                residual[s, c] = None
                gathered[s, c] = []
                for p in range(n_sub):
                    token[0] = first_norm(token[0], x_in, s, c * chunk_rows + p * sub_rows, sub_rows, ln_gain, ln_bias)
                    gathered[s, c].append(gather(token[0]))

        results, pending = {}, []

        def exchange_steps(layer_idx, s, c, keep, second):
            last = layer_idx == n_layers - 1
            third = []

            def step_one():
                token[0] = relay(token[0], keep, second)
                third.append(lax.ppermute(token[0], 'tp', hop_two))

            def step_two():
                raw = (s, c * chunk_rows) if residual[s, c] is None else None
                res = x_in if raw else residual[s, c]
                out = finish(token[0], layer_idx, last, keep, second, third[0], res, raw, b_out, b_down, ln_gain, ln_bias)
                if last:
                    results[s, c] = token[0] = out
                else:
                    residual[s, c], token[0] = out
                    gathered[s, c] = [gather(token[0])]

            return step_one, step_two

        def run_pending():
            if pending:
                for step in pending.pop(0):
                    step()

        for layer_idx in range(n_layers):
            for s in range(batch):
                qkv, ups, firsts = [], [[] for _ in range(n_chunks)], []
                for c in range(n_chunks):
                    for g in gathered[s, c]:
                        token[0] = qkv_project(token[0], layer_idx, g, w_qkv)
                        qkv.append(token[0])
                        run_pending()
                        token[0] = up_project(token[0], layer_idx, g, w_up, b_up)
                        ups[c].append(token[0])
                        run_pending()
                attn_out = token[0] = attention(token[0], qkv, tp_size)
                for c in range(n_chunks):
                    token[0] = project(token[0], layer_idx, c, n_chunks, other_table, ups[c], attn_out, w_down, w_out)
                    firsts.append(lax.ppermute(token[0], 'tp', partner))
                chunk_steps = []
                for c in range(n_chunks):
                    keep, token[0] = project(token[0], layer_idx, c, n_chunks, mine_table, ups[c], attn_out, w_down, w_out,
                                             firsts[c])
                    chunk_steps.append(exchange_steps(layer_idx, s, c, keep, lax.ppermute(token[0], 'tp', hop_one)))
                pending += [[chunk_steps[0][0]], [chunk_steps[1][0], chunk_steps[0][1]], [chunk_steps[1][1]]]
        while pending:
            run_pending()
        return jnp.stack([jnp.concatenate([results[s, c] for c in range(n_chunks)]) for s in range(batch)])

    in_specs = (act_spec, P(), P(), P(None, None, None, 'tp', None), P(None, 'tp', None, None), P(),
                P(None, None, 'tp'), P(None, 'tp'), P(None, 'tp', None), P())
    return jax.shard_map(local_fn, mesh=mesh, in_specs=in_specs, out_specs=act_spec, check_vma=False)
```

```python
import functools
import math

import jax
import jax.numpy as jnp
from jax import lax
from jax.experimental import pallas as pl
from jax.experimental.pallas import tpu as pltpu
from jax.sharding import PartitionSpec as P

LN_EPS = 1e-5
VMEM_LIMIT = 67043328
ANY = pl.BlockSpec(memory_space=pl.ANY)
PARAMS = pltpu.CompilerParams(vmem_limit_bytes=VMEM_LIMIT)


def norm_rows(row, gain, bias):
    row_mean = jnp.mean(row, axis=-1, keepdims=True)
    centered = row - row_mean
    row_var = jnp.mean(centered * centered, axis=-1, keepdims=True)
    return (centered * lax.rsqrt(row_var + LN_EPS) * gain + bias).astype(jnp.bfloat16)


def ln_kernel(token_ref, x_ref, gain_ref, bias_ref, h_ref):
    del token_ref
    h_ref[...] = norm_rows(x_ref[0].astype(jnp.float32), gain_ref[0], bias_ref[0])


def first_norm(token, x, seq, row, rows, ln_gain, ln_bias):
    width = x.shape[-1]
    tile = 32
    first = row // tile
    vec = pl.BlockSpec((1, 1, width), lambda i: (0, 0, 0))
    return pl.pallas_call(
        ln_kernel,
        grid=(rows // tile,),
        in_specs=[ANY, pl.BlockSpec((1, tile, width), lambda i: (seq, first + i, 0)), vec, vec],
        out_specs=pl.BlockSpec((tile, width), lambda i: (i, 0)),
        out_shape=jax.ShapeDtypeStruct((rows, width), jnp.bfloat16),
        compiler_params=PARAMS,
        cost_estimate=pl.CostEstimate(flops=rows * width * 20, bytes_accessed=rows * width * 4, transcendentals=0),
        name="first_norm",
    )(token, x, ln_gain, ln_bias)


def relay_kernel(token_ref, keep_ref, second_ref, out_ref):
    del token_ref
    out_ref[...] = (keep_ref[...] + second_ref[...].astype(jnp.float32)).astype(jnp.bfloat16)


def relay(token, keep, second):
    rows, width = keep.shape[0] // 2, keep.shape[1]
    tile = 64
    first = rows // tile
    data = pl.BlockSpec((tile, width), lambda i: (first + i, 0))
    return pl.pallas_call(
        relay_kernel,
        grid=(rows // tile,),
        in_specs=[ANY, data, data],
        out_specs=pl.BlockSpec((tile, width), lambda i: (i, 0)),
        out_shape=jax.ShapeDtypeStruct((rows, width), jnp.bfloat16),
        compiler_params=PARAMS,
        cost_estimate=pl.CostEstimate(flops=rows * width * 10, bytes_accessed=rows * width * 8, transcendentals=0),
        name="relay",
    )(token, keep, second)


def finish_kernel(last, raw, filled, token_ref, keep_ref, second_ref, third_ref, res_ref, b_out_ref, b_down_ref, *rest):
    del token_ref
    if filled:
        rest = rest[1:]
    summed = keep_ref[...] + second_ref[...].astype(jnp.float32) + third_ref[...].astype(jnp.float32)
    residual = res_ref[0].astype(jnp.float32) if raw else res_ref[...]
    row = residual + (summed + (b_out_ref[0] + b_down_ref[0]))
    if last:
        rest[0][0] = row.astype(jnp.bfloat16)
    else:
        gain_ref, bias_ref, h_ref, new_res_ref = rest
        new_res_ref[...] = row
        h_ref[...] = norm_rows(row, gain_ref[0], bias_ref[0])


def finish(token, layer_idx, last, seq, row, keep, second, third, residual, x_in, filled, b_out, b_down, ln_gain, ln_bias):
    rows, width = third.shape
    tile = 32
    first = row // tile
    data = pl.BlockSpec((tile, width), lambda i: (i, 0))
    raw = residual is None
    res_spec = pl.BlockSpec((1, tile, width), lambda i: (seq, first + i, 0)) if raw else data
    vec = pl.BlockSpec((1, 1, width), lambda i: (layer_idx, 0, 0))
    next_vec = pl.BlockSpec((1, 1, width), lambda i: (layer_idx + 1, 0, 0))
    args = [token, keep, second, third, x_in if raw else residual, b_out, b_down]
    in_specs = [ANY] + [data] * 3 + [res_spec] + [vec] * 2
    aliases = {}
    if filled is not None:
        aliases = {len(args): 0}
        args.append(filled)
        in_specs.append(ANY)
    if last:
        out_shape = jax.ShapeDtypeStruct(x_in.shape, jnp.bfloat16)
        out_specs = pl.BlockSpec((1, tile, width), lambda i: (seq, first + i, 0))
    else:
        args += [ln_gain, ln_bias]
        in_specs += [next_vec] * 2
        out_shape = (jax.ShapeDtypeStruct(x_in.shape[1:], jnp.bfloat16), jax.ShapeDtypeStruct((rows, width), jnp.float32))
        out_specs = (pl.BlockSpec((tile, width), lambda i: (first + i, 0)), data)
    return pl.pallas_call(
        functools.partial(finish_kernel, last, raw, filled is not None),
        grid=(rows // tile,),
        in_specs=in_specs,
        out_specs=out_specs,
        out_shape=out_shape,
        input_output_aliases=aliases,
        compiler_params=PARAMS,
        cost_estimate=pl.CostEstimate(flops=rows * width * 30, bytes_accessed=rows * width * 16, transcendentals=0),
        name="finish",
    )(*args)


SLICE = 256


def sliced_matmul(x_hbm, x_first, x_all, sems, right, store):
    n_slices = x_all.shape[0] // SLICE

    def fetch(k):
        return pltpu.make_async_copy(x_hbm.at[pl.ds(x_first + k * SLICE, SLICE)], x_all.at[pl.ds(k * SLICE, SLICE)], sems.at[k])

    def multiply(row):
        rows = x_all[pl.ds(row, SLICE), :]
        store(row, jnp.dot(rows, right(), preferred_element_type=jnp.float32))

    @pl.when(pl.program_id(0) == 0)
    def _():
        for k in range(n_slices):
            fetch(k).start()

        def arrived(k, carry):
            fetch(k).wait()
            multiply(pl.multiple_of(k * SLICE, SLICE))
            return carry

        lax.fori_loop(0, n_slices, arrived, 0)

    @pl.when(pl.program_id(0) > 0)
    def _():
        def several(group, carry):
            for k in range(4):
                multiply(pl.multiple_of((group * 4 + k) * SLICE, SLICE))
            return carry

        lax.fori_loop(0, n_slices // 4, several, 0)


def qkv_kernel(group, token_ref, x_hbm, w_ref, out_ref, x_all, sems):
    del token_ref
    head_dim = w_ref.shape[-1]

    def right():
        return jnp.concatenate([w_ref[0, i] for i in range(group)], axis=1)

    def store(row, value):
        for i in range(group):
            out_ref[i, pl.ds(row, SLICE), :] = value[:, i * head_dim:(i + 1) * head_dim].astype(jnp.bfloat16)

    sliced_matmul(x_hbm, 0, x_all, sems, right, store)


def qkv_project(token, layer_idx, x, w_qkv):
    rows, depth = x.shape
    _, slabs, _, head_dim = w_qkv.shape
    group = 4
    return pl.pallas_call(
        functools.partial(qkv_kernel, group),
        grid=(pl.cdiv(slabs, group),),
        in_specs=[ANY, ANY, pl.BlockSpec((1, group, depth, head_dim), lambda j: (layer_idx, j, 0, 0))],
        out_specs=pl.BlockSpec((group, rows, head_dim), lambda j: (j, 0, 0)),
        out_shape=jax.ShapeDtypeStruct((slabs, rows, head_dim), jnp.bfloat16),
        scratch_shapes=[pltpu.VMEM((rows, depth), jnp.bfloat16), pltpu.SemaphoreType.DMA((rows // SLICE,))],
        compiler_params=PARAMS,
        cost_estimate=pl.CostEstimate(flops=2 * rows * depth * slabs * head_dim, bytes_accessed=2 * depth * slabs * head_dim,
                                      transcendentals=0),
        name="qkv_project",
    )(token, x, w_qkv)


def up_kernel(x_first, token_ref, x_hbm, w_ref, b_ref, *rest):
    del token_ref
    out_ref, x_all, sems = rest[-3:]

    def store(row, value):
        hidden = value + b_ref[0]
        inner = math.sqrt(2 / math.pi) * (hidden + 0.044715 * (hidden * hidden * hidden))
        out_ref[pl.ds(row, SLICE), :] = (hidden * (0.5 * (1.0 + jnp.tanh(inner)))).astype(jnp.bfloat16)

    sliced_matmul(x_hbm, x_first, x_all, sems, lambda: w_ref[0], store)


def up_project(token, layer_idx, x, part, n_parts, filled, w_up, b_up):
    depth = x.shape[1]
    rows = x.shape[0] // n_parts
    width = w_up.shape[-1]
    tile = 512
    args = [token, x, w_up, b_up]
    in_specs = [ANY, ANY, pl.BlockSpec((1, depth, tile), lambda j: (layer_idx, 0, j)),
                pl.BlockSpec((1, 1, tile), lambda j: (layer_idx, 0, j))]
    aliases = {}
    if filled is not None:
        aliases = {len(args): 0}
        args.append(filled)
        in_specs.append(ANY)
    return pl.pallas_call(
        functools.partial(up_kernel, part * rows),
        grid=(width // tile,),
        in_specs=in_specs,
        out_specs=pl.BlockSpec((rows, tile), lambda j: (part, j)),
        out_shape=jax.ShapeDtypeStruct((x.shape[0], width), jnp.bfloat16),
        input_output_aliases=aliases,
        scratch_shapes=[pltpu.VMEM((rows, depth), jnp.bfloat16), pltpu.SemaphoreType.DMA((rows // SLICE,))],
        compiler_params=PARAMS,
        cost_estimate=pl.CostEstimate(flops=2 * rows * depth * width, bytes_accessed=2 * depth * width,
                                      transcendentals=rows * width),
        name="up_project",
    )(*args)


def attention_kernel(n_chunks, q_tile, token_ref, *refs):
    del token_ref
    parts = [refs[3 * c:3 * c + 3] for c in range(n_chunks)]
    out_ref, q_all, k_all, v_all = refs[3 * n_chunks:]
    for c in range(n_chunks):
        for whole, part in zip((q_all, k_all, v_all), parts[c]):
            whole[:, c] = part[0]
    blocks, _, rows, head_dim = q_all.shape
    seq_len = blocks * n_chunks * rows
    exp_scale = head_dim ** -0.5 * math.log2(math.e)
    queries = q_all[...].reshape(seq_len, head_dim)
    keys = k_all[...].reshape(seq_len, head_dim)
    values = v_all[...].reshape(seq_len, head_dim)
    causal = (lax.broadcasted_iota(jnp.int32, (q_tile, q_tile), 1) <= lax.broadcasted_iota(jnp.int32, (q_tile, q_tile), 0))
    nt = (((1,), (1,)), ((), ()))
    for tile in range(seq_len // q_tile):
        start, stop = tile * q_tile, (tile + 1) * q_tile
        query = queries[start:stop]
        diag = lax.dot_general(query, keys[start:stop], nt, preferred_element_type=jnp.float32)
        diag = jnp.where(causal, diag, -jnp.inf)
        top = jnp.max(diag, axis=1, keepdims=True)
        if tile:
            past = lax.dot_general(query, keys[:start], nt, preferred_element_type=jnp.float32)
            top = jnp.maximum(top, jnp.max(past, axis=1, keepdims=True))
        diag = jnp.exp2((diag - top) * exp_scale)
        total = jnp.sum(diag, axis=1, keepdims=True)
        if tile:
            past = jnp.exp2((past - top) * exp_scale)
            total = total + jnp.sum(past, axis=1, keepdims=True)
        inverse = 1.0 / total
        out = jnp.dot((diag * inverse).astype(jnp.bfloat16), values[start:stop], preferred_element_type=jnp.float32)
        if tile:
            out = out + jnp.dot((past * inverse).astype(jnp.bfloat16), values[:start], preferred_element_type=jnp.float32)
        out_ref[start:stop, :] = out.astype(jnp.bfloat16)


def attention(token, qkv_chunks, blocks):
    n_chunks = len(qkv_chunks)
    slabs, all_rows, head_dim = qkv_chunks[0].shape
    heads, rows = slabs // 3, all_rows // blocks
    seq_len = all_rows * n_chunks
    specs = [pl.BlockSpec((1, blocks, rows, head_dim), lambda h, t=t: (t * heads + h, 0, 0, 0)) for t in range(3)]
    args = [chunk.reshape(slabs, blocks, rows, head_dim) for chunk in qkv_chunks for _ in range(3)]
    whole = pltpu.VMEM((blocks, n_chunks, rows, head_dim), jnp.bfloat16)
    return pl.pallas_call(
        functools.partial(attention_kernel, n_chunks, 256),
        grid=(heads,),
        in_specs=[ANY] + specs * n_chunks,
        out_specs=pl.BlockSpec((seq_len, head_dim), lambda h: (0, h)),
        out_shape=jax.ShapeDtypeStruct((seq_len, heads * head_dim), jnp.bfloat16),
        scratch_shapes=[whole] * 3,
        compiler_params=PARAMS,
        cost_estimate=pl.CostEstimate(flops=heads * seq_len * seq_len * head_dim * 8,
                                      bytes_accessed=heads * seq_len * head_dim * 8, transcendentals=0),
        name="attention",
    )(token, *args)


def project_kernel(mine, table_ref, token_ref, *refs):
    del table_ref, token_ref
    u_refs, o_refs, w_down_ref, w_out_ref, refs = refs[:4], refs[4:8], refs[8], refs[9], refs[10:]
    left = refs[-1]
    depth = u_refs[0].shape[1]
    all_rows = left.shape[0]

    @pl.when(pl.program_id(0) == 0)
    def _():
        rows = all_rows // 4
        for k in range(4):
            left[k * rows:(k + 1) * rows, :depth] = u_refs[k][...]
            left[k * rows:(k + 1) * rows, depth:] = o_refs[k][0, 0]

    step = all_rows // 2
    for row in (0, step):
        right = jnp.concatenate([w_down_ref[0], w_out_ref[0]], axis=0)
        partial = jnp.dot(left[row:row + step, :], right, preferred_element_type=jnp.float32)
        if mine:
            first_ref, keep_ref, send_ref = refs[:3]
            partial = partial + first_ref[row:row + step, :].astype(jnp.float32)
            if row == 0:
                keep_ref[...] = partial
            else:
                send_ref[...] = partial.astype(jnp.bfloat16)
        else:
            refs[0][row:row + step, :] = partial.astype(jnp.bfloat16)


def project(token, layer_idx, chunk, n_chunks, table, u, attn_out, w_down, w_out, first=None):
    seq_len, heads_width = attn_out.shape
    rows = seq_len // 8 // n_chunks
    stride, offset = (n_chunks, chunk) if u.shape[0] == seq_len else (1, 0)
    depth, width = w_down.shape[1:]
    attn_blocks = attn_out.reshape(8, n_chunks, rows, heads_width)
    tile = 512
    in_specs, args = [ANY], [token]
    for k in range(4):
        in_specs.append(pl.BlockSpec((rows, depth), lambda j, tbl, k=k: (tbl[k] * stride + offset, 0)))
        args.append(u)
    for k in range(4):
        in_specs.append(pl.BlockSpec((1, 1, rows, heads_width), lambda j, tbl, k=k: (tbl[k], chunk, 0, 0)))
        args.append(attn_blocks)
    in_specs.append(pl.BlockSpec((1, depth, tile), lambda j, tbl: (layer_idx, 0, j)))
    in_specs.append(pl.BlockSpec((1, heads_width, tile), lambda j, tbl: (layer_idx, 0, j)))
    args += [w_down, w_out]
    all_rows = 4 * rows
    if first is None:
        out_shape = jax.ShapeDtypeStruct((all_rows, width), jnp.bfloat16)
        out_specs = pl.BlockSpec((all_rows, tile), lambda j, tbl: (0, j))
    else:
        in_specs.append(pl.BlockSpec((all_rows, tile), lambda j, tbl: (0, j)))
        args.append(first)
        out_shape = (jax.ShapeDtypeStruct((all_rows // 2, width), jnp.float32),
                     jax.ShapeDtypeStruct((all_rows // 2, width), jnp.bfloat16))
        out_specs = (pl.BlockSpec((all_rows // 2, tile), lambda j, tbl: (0, j)),) * 2
    return pl.pallas_call(
        functools.partial(project_kernel, first is not None),
        grid_spec=pltpu.PrefetchScalarGridSpec(
            num_scalar_prefetch=1,
            grid=(width // tile,),
            in_specs=in_specs,
            out_specs=out_specs,
            scratch_shapes=[pltpu.VMEM((all_rows, depth + heads_width), jnp.bfloat16)],
        ),
        out_shape=out_shape,
        compiler_params=PARAMS,
        cost_estimate=pl.CostEstimate(flops=2 * all_rows * (depth + heads_width) * width,
                                      bytes_accessed=2 * (depth + heads_width) * width, transcendentals=0),
        name="project",
    )(table, *args)


def solution(mesh):
    tp_size = mesh.shape['tp']
    act_spec = P('dp', 'tp', None)
    partner = [(i, i ^ 1) for i in range(tp_size)]
    hop_one = [(i, i ^ (2 if i & 1 else 4)) for i in range(tp_size)]
    hop_two = [(i, i ^ (4 if i & 1 else 2)) for i in range(tp_size)]

    def local_fn(x_in, ln_gain, ln_bias, w_qkv, w_out, b_out, w_up, b_up, w_down, b_down):
        batch, local_rows, width = x_in.shape
        n_layers, _, _, heads, head_dim = w_qkv.shape
        vec = lambda a: a.reshape(n_layers, 1, a.shape[1])
        ln_gain, ln_bias, b_out, b_down, b_up = vec(ln_gain), vec(ln_bias), vec(b_out), vec(b_down), vec(b_up)
        w_out = w_out.reshape(n_layers, heads * head_dim, width)
        w_qkv = jnp.transpose(w_qkv, (0, 2, 3, 1, 4)).reshape(n_layers, 3 * heads, width, head_dim)
        me = lax.axis_index('tp').astype(jnp.int32)
        bit_one = jnp.where((me & 1) == 1, 2, 4)
        bit_two = 6 - bit_one
        steps = jnp.array([0, 0, 1, 1], jnp.int32), jnp.array([0, 1, 0, 1], jnp.int32)
        mine_table = (me ^ (steps[0] * bit_one) ^ (steps[1] * bit_two)).astype(jnp.int32)
        other_table = (me ^ 1 ^ (steps[0] * bit_two) ^ (steps[1] * bit_one)).astype(jnp.int32)

        n_chunks = 2
        chunk_rows = local_rows // n_chunks
        token = [x_in]

        def gather(h):
            return lax.all_gather(h, 'tp', axis=0, tiled=True)

        gathered = []
        for s in range(batch):
            parts = n_chunks if s == 0 else 1
            rows = local_rows // parts
            gathered.append([])
            for p in range(parts):
                token[0] = first_norm(token[0], x_in, s, p * rows, rows, ln_gain, ln_bias)
                gathered[s].append(gather(token[0]))

        residual, filled, pending = {}, [None], []

        def exchange_steps(layer_idx, s, c, keep, second):
            last = layer_idx == n_layers - 1
            third = []

            def step_one():
                token[0] = relay(token[0], keep, second)
                third.append(lax.ppermute(token[0], 'tp', hop_two))

            def step_two():
                out = finish(token[0], layer_idx, last, s, c * chunk_rows, keep, second, third[0], residual.get((s, c)), x_in,
                             filled[0], b_out, b_down, ln_gain, ln_bias)
                if last:
                    filled[0] = token[0] = out
                else:
                    token[0], residual[s, c] = out
                    if c == n_chunks - 1:
                        gathered[s] = [gather(token[0])]
                    filled[0] = None if c == n_chunks - 1 else token[0]

            return step_one, step_two

        def run_pending():
            if pending:
                for step in pending.pop(0):
                    step()

        for layer_idx in range(n_layers):
            for s in range(batch):
                qkv, ups = [], []
                pieces = gathered[s]
                for g in pieces:
                    token[0] = qkv_project(token[0], layer_idx, g, w_qkv)
                    qkv.append(token[0])
                    run_pending()
                    n_parts = 3 - len(pieces)
                    out = None
                    for part in range(n_parts):
                        out = token[0] = up_project(token[0], layer_idx, g, part, n_parts, out, w_up, b_up)
                        run_pending()
                    ups.append(out)
                attn_out = token[0] = attention(token[0], qkv, tp_size)
                firsts, chunk_steps = [], []
                for c in range(n_chunks):
                    token[0] = project(token[0], layer_idx, c, n_chunks, other_table, ups[c % len(ups)], attn_out, w_down, w_out)
                    firsts.append(lax.ppermute(token[0], 'tp', partner))
                for c in range(n_chunks):
                    keep, token[0] = project(token[0], layer_idx, c, n_chunks, mine_table, ups[c % len(ups)], attn_out, w_down,
                                             w_out, firsts[c])
                    chunk_steps.append(exchange_steps(layer_idx, s, c, keep, lax.ppermute(token[0], 'tp', hop_one)))
                if layer_idx == n_layers - 1 and s == batch - 1:
                    pending += [[chunk_steps[0][0], chunk_steps[1][0], chunk_steps[0][1], chunk_steps[1][1]]]
                else:
                    pending += [[chunk_steps[0][0], chunk_steps[1][0]], [chunk_steps[0][1], chunk_steps[1][1]]]
        run_pending()
        return filled[0]

    in_specs = (act_spec, P(), P(), P(None, None, None, 'tp', None), P(None, 'tp', None, None), P(),
                P(None, None, 'tp'), P(None, 'tp'), P(None, 'tp', None), P())
    return jax.shard_map(local_fn, mesh=mesh, in_specs=in_specs, out_specs=act_spec, check_vma=False)
```

```python
import functools
import math

import jax
import jax.numpy as jnp
from jax import lax
from jax.experimental import pallas as pl
from jax.experimental.pallas import tpu as pltpu
from jax.sharding import PartitionSpec as P

LN_EPS = 1e-5
VMEM_LIMIT = 67043328
ANY = pl.BlockSpec(memory_space=pl.ANY)
PARAMS = pltpu.CompilerParams(vmem_limit_bytes=VMEM_LIMIT)


def norm_rows(row, gain, bias):
    row_mean = jnp.mean(row, axis=-1, keepdims=True)
    centered = row - row_mean
    row_var = jnp.mean(centered * centered, axis=-1, keepdims=True)
    return (centered * lax.rsqrt(row_var + LN_EPS) * gain + bias).astype(jnp.bfloat16)


def ln_kernel(token_ref, x_ref, gain_ref, bias_ref, h_ref):
    del token_ref
    h_ref[...] = norm_rows(x_ref[0].astype(jnp.float32), gain_ref[0], bias_ref[0])


def first_norm(token, x, seq, row, rows, ln_gain, ln_bias):
    width = x.shape[-1]
    tile = 32
    first = row // tile
    vec = pl.BlockSpec((1, 1, width), lambda i: (0, 0, 0))
    return pl.pallas_call(
        ln_kernel,
        grid=(rows // tile,),
        in_specs=[ANY, pl.BlockSpec((1, tile, width), lambda i: (seq, first + i, 0)), vec, vec],
        out_specs=pl.BlockSpec((tile, width), lambda i: (i, 0)),
        out_shape=jax.ShapeDtypeStruct((rows, width), jnp.bfloat16),
        compiler_params=PARAMS,
        cost_estimate=pl.CostEstimate(flops=rows * width * 20, bytes_accessed=rows * width * 4, transcendentals=0),
        name="first_norm",
    )(token, x, ln_gain, ln_bias)


def relay_kernel(token_ref, keep_ref, second_ref, out_ref):
    del token_ref
    out_ref[...] = (keep_ref[...] + second_ref[...].astype(jnp.float32)).astype(jnp.bfloat16)


def relay(token, keep, second):
    rows, width = keep.shape[0] // 2, keep.shape[1]
    tile = 64
    first = rows // tile
    data = pl.BlockSpec((tile, width), lambda i: (first + i, 0))
    return pl.pallas_call(
        relay_kernel,
        grid=(rows // tile,),
        in_specs=[ANY, data, data],
        out_specs=pl.BlockSpec((tile, width), lambda i: (i, 0)),
        out_shape=jax.ShapeDtypeStruct((rows, width), jnp.bfloat16),
        compiler_params=PARAMS,
        cost_estimate=pl.CostEstimate(flops=rows * width * 10, bytes_accessed=rows * width * 8, transcendentals=0),
        name="relay",
    )(token, keep, second)


def finish_kernel(last, raw, filled, token_ref, keep_ref, second_ref, third_ref, res_ref, b_out_ref, b_down_ref, *rest):
    del token_ref
    if filled:
        rest = rest[1:]
    summed = keep_ref[...] + second_ref[...].astype(jnp.float32) + third_ref[...].astype(jnp.float32)
    residual = res_ref[0].astype(jnp.float32) if raw else res_ref[...]
    row = residual + (summed + (b_out_ref[0] + b_down_ref[0]))
    if last:
        rest[0][0] = row.astype(jnp.bfloat16)
    else:
        gain_ref, bias_ref, h_ref, new_res_ref = rest
        new_res_ref[...] = row
        h_ref[...] = norm_rows(row, gain_ref[0], bias_ref[0])


def finish(token, layer_idx, last, seq, row, keep, second, third, residual, x_in, filled, b_out, b_down, ln_gain, ln_bias):
    rows, width = third.shape
    tile = 32
    first = row // tile
    data = pl.BlockSpec((tile, width), lambda i: (i, 0))
    raw = residual is None
    res_spec = pl.BlockSpec((1, tile, width), lambda i: (seq, first + i, 0)) if raw else data
    vec = pl.BlockSpec((1, 1, width), lambda i: (layer_idx, 0, 0))
    next_vec = pl.BlockSpec((1, 1, width), lambda i: (layer_idx + 1, 0, 0))
    args = [token, keep, second, third, x_in if raw else residual, b_out, b_down]
    in_specs = [ANY] + [data] * 3 + [res_spec] + [vec] * 2
    aliases = {}
    if filled is not None:
        aliases = {len(args): 0}
        args.append(filled)
        in_specs.append(ANY)
    if last:
        out_shape = jax.ShapeDtypeStruct(x_in.shape, jnp.bfloat16)
        out_specs = pl.BlockSpec((1, tile, width), lambda i: (seq, first + i, 0))
    else:
        args += [ln_gain, ln_bias]
        in_specs += [next_vec] * 2
        out_shape = (jax.ShapeDtypeStruct(x_in.shape[1:], jnp.bfloat16), jax.ShapeDtypeStruct((rows, width), jnp.float32))
        out_specs = (pl.BlockSpec((tile, width), lambda i: (first + i, 0)), data)
    return pl.pallas_call(
        functools.partial(finish_kernel, last, raw, filled is not None),
        grid=(rows // tile,),
        in_specs=in_specs,
        out_specs=out_specs,
        out_shape=out_shape,
        input_output_aliases=aliases,
        compiler_params=PARAMS,
        cost_estimate=pl.CostEstimate(flops=rows * width * 30, bytes_accessed=rows * width * 16, transcendentals=0),
        name="finish",
    )(*args)


SLICE = 256


def sliced_matmul(x_hbm, x_first, x_all, sems, right, store):
    n_slices = x_all.shape[0] // SLICE

    def fetch(k):
        return pltpu.make_async_copy(x_hbm.at[pl.ds(x_first + k * SLICE, SLICE)], x_all.at[pl.ds(k * SLICE, SLICE)], sems.at[k])

    def multiply(row):
        rows = x_all[pl.ds(row, SLICE), :]
        store(row, jnp.dot(rows, right(), preferred_element_type=jnp.float32))

    @pl.when(pl.program_id(0) == 0)
    def _():
        fetch(0).start()
        fetch(1).start()

        def arrived(k, carry):
            fetch(k).wait()

            @pl.when(k + 2 < n_slices)
            def _():
                fetch(k + 2).start()

            multiply(pl.multiple_of(k * SLICE, SLICE))
            return carry

        lax.fori_loop(0, n_slices, arrived, 0)

    @pl.when(pl.program_id(0) > 0)
    def _():
        def several(group, carry):
            for k in range(4):
                multiply(pl.multiple_of((group * 4 + k) * SLICE, SLICE))
            return carry

        lax.fori_loop(0, n_slices // 4, several, 0)


def qkv_kernel(group, token_ref, x_hbm, w_ref, out_ref, x_all, sems):
    del token_ref
    head_dim = w_ref.shape[-1]

    def right():
        return jnp.concatenate([w_ref[0, i] for i in range(group)], axis=1)

    def store(row, value):
        for i in range(group):
            out_ref[i, pl.ds(row, SLICE), :] = value[:, i * head_dim:(i + 1) * head_dim].astype(jnp.bfloat16)

    sliced_matmul(x_hbm, 0, x_all, sems, right, store)


def qkv_project(token, layer_idx, x, w_qkv):
    rows, depth = x.shape
    _, slabs, _, head_dim = w_qkv.shape
    group = 4
    return pl.pallas_call(
        functools.partial(qkv_kernel, group),
        grid=(pl.cdiv(slabs, group),),
        in_specs=[ANY, ANY, pl.BlockSpec((1, group, depth, head_dim), lambda j: (layer_idx, j, 0, 0))],
        out_specs=pl.BlockSpec((group, rows, head_dim), lambda j: (j, 0, 0)),
        out_shape=jax.ShapeDtypeStruct((slabs, rows, head_dim), jnp.bfloat16),
        scratch_shapes=[pltpu.VMEM((rows, depth), jnp.bfloat16), pltpu.SemaphoreType.DMA((rows // SLICE,))],
        compiler_params=PARAMS,
        cost_estimate=pl.CostEstimate(flops=2 * rows * depth * slabs * head_dim, bytes_accessed=2 * depth * slabs * head_dim,
                                      transcendentals=0),
        name="qkv_project",
    )(token, x, w_qkv)


def up_kernel(x_first, token_ref, x_hbm, w_ref, b_ref, *rest):
    del token_ref
    out_ref, x_all, sems = rest[-3:]

    def store(row, value):
        hidden = value + b_ref[0]
        inner = math.sqrt(2 / math.pi) * (hidden + 0.044715 * (hidden * hidden * hidden))
        out_ref[pl.ds(row, SLICE), :] = (hidden * (0.5 * (1.0 + jnp.tanh(inner)))).astype(jnp.bfloat16)

    sliced_matmul(x_hbm, x_first, x_all, sems, lambda: w_ref[0], store)


def up_project(token, layer_idx, x, part, n_parts, filled, w_up, b_up):
    depth = x.shape[1]
    rows = x.shape[0] // n_parts
    width = w_up.shape[-1]
    tile = 512
    args = [token, x, w_up, b_up]
    in_specs = [ANY, ANY, pl.BlockSpec((1, depth, tile), lambda j: (layer_idx, 0, j)),
                pl.BlockSpec((1, 1, tile), lambda j: (layer_idx, 0, j))]
    aliases = {}
    if filled is not None:
        aliases = {len(args): 0}
        args.append(filled)
        in_specs.append(ANY)
    return pl.pallas_call(
        functools.partial(up_kernel, part * rows),
        grid=(width // tile,),
        in_specs=in_specs,
        out_specs=pl.BlockSpec((rows, tile), lambda j: (part, j)),
        out_shape=jax.ShapeDtypeStruct((x.shape[0], width), jnp.bfloat16),
        input_output_aliases=aliases,
        scratch_shapes=[pltpu.VMEM((rows, depth), jnp.bfloat16), pltpu.SemaphoreType.DMA((rows // SLICE,))],
        compiler_params=PARAMS,
        cost_estimate=pl.CostEstimate(flops=2 * rows * depth * width, bytes_accessed=2 * depth * width,
                                      transcendentals=rows * width),
        name="up_project",
    )(*args)


def attention_kernel(n_chunks, q_tile, token_ref, *refs):
    del token_ref
    parts = [refs[3 * c:3 * c + 3] for c in range(n_chunks)]
    out_ref, q_all, k_all, v_all, score_all = refs[3 * n_chunks:]
    for c in range(n_chunks):
        for whole, part in zip((q_all, k_all, v_all), parts[c]):
            whole[:, c] = part[0]
    blocks, _, rows, head_dim = q_all.shape
    seq_len = blocks * n_chunks * rows
    exp_scale = head_dim ** -0.5 * math.log2(math.e)
    queries = q_all[...].reshape(seq_len, head_dim)
    keys = k_all[...].reshape(seq_len, head_dim)
    values = v_all[...].reshape(seq_len, head_dim)
    causal = (lax.broadcasted_iota(jnp.int32, (q_tile, q_tile), 1) <= lax.broadcasted_iota(jnp.int32, (q_tile, q_tile), 0))
    nt = (((1,), (1,)), ((), ()))

    def scores(tile):
        start, stop = tile * q_tile, (tile + 1) * q_tile
        score = lax.dot_general(queries[start:stop], keys[:stop], nt, preferred_element_type=jnp.float32)
        diag = jnp.where(causal, score[:, start:], -jnp.inf)
        score_all[tile % 2, :, start:stop] = diag
        if tile:
            score_all[tile % 2, :, :start] = score[:, :start]
            diag = jnp.concatenate([score[:, :start], diag], axis=1)
        return jnp.max(diag, axis=1, keepdims=True)

    n_tiles = seq_len // q_tile
    top = scores(0)
    for tile in range(n_tiles):
        next_top = scores(tile + 1) if tile + 1 < n_tiles else None
        start, stop = tile * q_tile, (tile + 1) * q_tile
        weight = jnp.exp2((score_all[tile % 2, :, :stop] - top) * exp_scale)
        score_all[tile % 2, :, :stop] = weight
        inverse = 1.0 / jnp.sum(weight, axis=1, keepdims=True)
        prob = (score_all[tile % 2, :, :stop] * inverse).astype(jnp.bfloat16)
        out = jnp.dot(prob, values[:stop], preferred_element_type=jnp.float32)
        out_ref[start:stop, :] = out.astype(jnp.bfloat16)
        top = next_top


def attention(token, qkv_chunks, blocks):
    n_chunks = len(qkv_chunks)
    slabs, all_rows, head_dim = qkv_chunks[0].shape
    heads, rows = slabs // 3, all_rows // blocks
    seq_len = all_rows * n_chunks
    specs = [pl.BlockSpec((1, blocks, rows, head_dim), lambda h, t=t: (t * heads + h, 0, 0, 0)) for t in range(3)]
    args = [chunk.reshape(slabs, blocks, rows, head_dim) for chunk in qkv_chunks for _ in range(3)]
    whole = pltpu.VMEM((blocks, n_chunks, rows, head_dim), jnp.bfloat16)
    return pl.pallas_call(
        functools.partial(attention_kernel, n_chunks, 256),
        grid=(heads,),
        in_specs=[ANY] + specs * n_chunks,
        out_specs=pl.BlockSpec((seq_len, head_dim), lambda h: (0, h)),
        out_shape=jax.ShapeDtypeStruct((seq_len, heads * head_dim), jnp.bfloat16),
        scratch_shapes=[whole] * 3 + [pltpu.VMEM((2, 256, seq_len), jnp.float32)],
        compiler_params=PARAMS,
        cost_estimate=pl.CostEstimate(flops=heads * seq_len * seq_len * head_dim * 8,
                                      bytes_accessed=heads * seq_len * head_dim * 8, transcendentals=0),
        name="attention",
    )(token, *args)


def project_kernel(mine, table_ref, token_ref, *refs):
    del table_ref, token_ref
    u_refs, o_refs, w_down_ref, w_out_ref, refs = refs[:4], refs[4:8], refs[8], refs[9], refs[10:]
    left = refs[-1]
    depth = u_refs[0].shape[1]
    all_rows = left.shape[0]

    @pl.when(pl.program_id(0) == 0)
    def _():
        rows = all_rows // 4
        for k in range(4):
            left[k * rows:(k + 1) * rows, :depth] = u_refs[k][...]
            left[k * rows:(k + 1) * rows, depth:] = o_refs[k][0, 0]

    step = all_rows // 2
    for row in (0, step):
        right = jnp.concatenate([w_down_ref[0], w_out_ref[0]], axis=0)
        partial = jnp.dot(left[row:row + step, :], right, preferred_element_type=jnp.float32)
        if mine:
            first_ref, keep_ref, send_ref = refs[:3]
            partial = partial + first_ref[row:row + step, :].astype(jnp.float32)
            if row == 0:
                keep_ref[...] = partial
            else:
                send_ref[...] = partial.astype(jnp.bfloat16)
        else:
            refs[0][row:row + step, :] = partial.astype(jnp.bfloat16)


def project(token, layer_idx, chunk, n_chunks, table, u, attn_out, w_down, w_out, first=None):
    seq_len, heads_width = attn_out.shape
    rows = seq_len // 8 // n_chunks
    stride, offset = (n_chunks, chunk) if u.shape[0] == seq_len else (1, 0)
    depth, width = w_down.shape[1:]
    attn_blocks = attn_out.reshape(8, n_chunks, rows, heads_width)
    tile = 512
    in_specs, args = [ANY], [token]
    for k in range(4):
        in_specs.append(pl.BlockSpec((rows, depth), lambda j, tbl, k=k: (tbl[k] * stride + offset, 0)))
        args.append(u)
    for k in range(4):
        in_specs.append(pl.BlockSpec((1, 1, rows, heads_width), lambda j, tbl, k=k: (tbl[k], chunk, 0, 0)))
        args.append(attn_blocks)
    in_specs.append(pl.BlockSpec((1, depth, tile), lambda j, tbl: (layer_idx, 0, j)))
    in_specs.append(pl.BlockSpec((1, heads_width, tile), lambda j, tbl: (layer_idx, 0, j)))
    args += [w_down, w_out]
    all_rows = 4 * rows
    if first is None:
        out_shape = jax.ShapeDtypeStruct((all_rows, width), jnp.bfloat16)
        out_specs = pl.BlockSpec((all_rows, tile), lambda j, tbl: (0, j))
    else:
        in_specs.append(pl.BlockSpec((all_rows, tile), lambda j, tbl: (0, j)))
        args.append(first)
        out_shape = (jax.ShapeDtypeStruct((all_rows // 2, width), jnp.float32),
                     jax.ShapeDtypeStruct((all_rows // 2, width), jnp.bfloat16))
        out_specs = (pl.BlockSpec((all_rows // 2, tile), lambda j, tbl: (0, j)),) * 2
    return pl.pallas_call(
        functools.partial(project_kernel, first is not None),
        grid_spec=pltpu.PrefetchScalarGridSpec(
            num_scalar_prefetch=1,
            grid=(width // tile,),
            in_specs=in_specs,
            out_specs=out_specs,
            scratch_shapes=[pltpu.VMEM((all_rows, depth + heads_width), jnp.bfloat16)],
        ),
        out_shape=out_shape,
        compiler_params=PARAMS,
        cost_estimate=pl.CostEstimate(flops=2 * all_rows * (depth + heads_width) * width,
                                      bytes_accessed=2 * (depth + heads_width) * width, transcendentals=0),
        name="project",
    )(table, *args)


def solution(mesh):
    tp_size = mesh.shape['tp']
    act_spec = P('dp', 'tp', None)
    partner = [(i, i ^ 1) for i in range(tp_size)]
    hop_one = [(i, i ^ (2 if i & 1 else 4)) for i in range(tp_size)]
    hop_two = [(i, i ^ (4 if i & 1 else 2)) for i in range(tp_size)]

    def local_fn(x_in, ln_gain, ln_bias, w_qkv, w_out, b_out, w_up, b_up, w_down, b_down):
        batch, local_rows, width = x_in.shape
        n_layers, _, _, heads, head_dim = w_qkv.shape
        vec = lambda a: a.reshape(n_layers, 1, a.shape[1])
        ln_gain, ln_bias, b_out, b_down, b_up = vec(ln_gain), vec(ln_bias), vec(b_out), vec(b_down), vec(b_up)
        w_out = w_out.reshape(n_layers, heads * head_dim, width)
        w_qkv = jnp.transpose(w_qkv, (0, 2, 3, 1, 4)).reshape(n_layers, 3 * heads, width, head_dim)
        me = lax.axis_index('tp').astype(jnp.int32)
        bit_one = jnp.where((me & 1) == 1, 2, 4)
        bit_two = 6 - bit_one
        steps = jnp.array([0, 0, 1, 1], jnp.int32), jnp.array([0, 1, 0, 1], jnp.int32)
        mine_table = (me ^ (steps[0] * bit_one) ^ (steps[1] * bit_two)).astype(jnp.int32)
        other_table = (me ^ 1 ^ (steps[0] * bit_two) ^ (steps[1] * bit_one)).astype(jnp.int32)

        n_chunks = 2
        chunk_rows = local_rows // n_chunks
        token = [x_in]

        def gather(h):
            return lax.all_gather(h, 'tp', axis=0, tiled=True)

        gathered = []
        for s in range(batch):
            parts = n_chunks if s == 0 else 1
            rows = local_rows // parts
            gathered.append([])
            for p in range(parts):
                token[0] = first_norm(token[0], x_in, s, p * rows, rows, ln_gain, ln_bias)
                gathered[s].append(gather(token[0]))

        residual, filled, pending = {}, [None], []

        def exchange_steps(layer_idx, s, c, keep, second):
            last = layer_idx == n_layers - 1
            third = []

            def step_one():
                token[0] = relay(token[0], keep, second)
                third.append(lax.ppermute(token[0], 'tp', hop_two))

            def step_two():
                out = finish(token[0] if c == 0 else third[0], layer_idx, last, s, c * chunk_rows, keep, second, third[0], residual.get((s, c)), x_in,
                             filled[0], b_out, b_down, ln_gain, ln_bias)
                if last:
                    filled[0] = token[0] = out
                else:
                    token[0], residual[s, c] = out
                    if c == n_chunks - 1:
                        gathered[s] = [gather(token[0])]
                    filled[0] = None if c == n_chunks - 1 else token[0]

            return step_one, step_two

        def run_pending():
            if pending:
                for step in pending.pop(0):
                    step()

        for layer_idx in range(n_layers):
            for s in range(batch):
                qkv, ups = [], []
                pieces = gathered[s]
                for g in pieces:
                    token[0] = qkv_project(token[0], layer_idx, g, w_qkv)
                    qkv.append(token[0])
                    run_pending()
                    n_parts = 3 - len(pieces)
                    out = None
                    for part in range(n_parts):
                        out = token[0] = up_project(token[0], layer_idx, g, part, n_parts, out, w_up, b_up)
                        run_pending()
                    ups.append(out)
                attn_out = token[0] = attention(token[0], qkv, tp_size)
                firsts, chunk_steps = [], []
                for c in range(n_chunks):
                    token[0] = project(token[0], layer_idx, c, n_chunks, other_table, ups[c % len(ups)], attn_out, w_down, w_out)
                    firsts.append(lax.ppermute(token[0], 'tp', partner))
                for c in range(n_chunks):
                    keep, token[0] = project(token[0], layer_idx, c, n_chunks, mine_table, ups[c % len(ups)], attn_out, w_down,
                                             w_out, firsts[c])
                    chunk_steps.append(exchange_steps(layer_idx, s, c, keep, lax.ppermute(token[0], 'tp', hop_one)))
                if layer_idx == n_layers - 1 and s == batch - 1:
                    pending += [[chunk_steps[0][0], chunk_steps[1][0], chunk_steps[0][1], chunk_steps[1][1]]]
                else:
                    pending += [[chunk_steps[0][0], chunk_steps[1][0]], [chunk_steps[0][1], chunk_steps[1][1]]]
        run_pending()
        return filled[0]

    in_specs = (act_spec, P(), P(), P(None, None, None, 'tp', None), P(None, 'tp', None, None), P(),
                P(None, None, 'tp'), P(None, 'tp'), P(None, 'tp', None), P())
    return jax.shard_map(local_fn, mesh=mesh, in_specs=in_specs, out_specs=act_spec, check_vma=False)
```
